8 devices in a mesh: dp: 1 (over z), w: 8 (over y, x, core).
Axes of the slice: x: 2, y: 2, z: 1, core: 2. Of those that a mesh axis runs over, the one named last changes fastest.
Arguments:
- hidden: bfloat16 [64, 256, 2048], P(('dp', 'w'))
- lengths: int32 [64], P(('dp', 'w'))
- attn_norm: bfloat16 [2, 2048], P(None, 'w')
- w_q: bfloat16 [2, 2048, 2048], P(None, 'w')
- w_k: bfloat16 [2, 2048, 256], P(None, 'w')
- w_v: bfloat16 [2, 2048, 256], P(None, 'w')
- w_o: bfloat16 [2, 2048, 2048], P(None, 'w')
- mlp_norm: bfloat16 [2, 2048], P(None, 'w')
- w_gate: bfloat16 [2, 2048, 16384], P(None, 'w')
- w_up: bfloat16 [2, 2048, 16384], P(None, 'w')
- w_down: bfloat16 [2, 16384, 2048], P(None, 'w')
Outputs:
- output 1: bfloat16 [64, 256, 2048], P(('dp', 'w'))
- output 2: bfloat16 [2, 64, 256, 1, 256], P(None, ('dp', 'w'))
- output 3: bfloat16 [2, 64, 256, 1, 256], P(None, ('dp', 'w'))
All inputs are finite; a program needn't handle non-finite values.
Results may differ from the reference program's by a relative error of at most 0.0138382.
Values are sent between devices in bfloat16 or wider.
A program may use at most 1 GiB of HBM per device.

```python
import jax
import jax.numpy as jnp
from jax import lax

D_MODEL = 2048
N_HEADS = 8
KV_HEADS = 1
HEAD_DIM = 256
D_FF = 16384
SEQ_LEN = 256
N_SEQS = 64
N_LAYERS = 2
RMS_EPS = 1e-6
ROPE_THETA = 10000.0
QUERY_BLOCK = min(SEQ_LEN, 512)
GROUP_SIZE = N_HEADS // KV_HEADS


def weight_draw(key_w, weight_shape, weight_scale):
    return (jax.random.normal(key_w, weight_shape, jnp.float32) * weight_scale).astype(jnp.bfloat16)


def setup_inputs(seed: int = 0, part: int = 0) -> dict:
    part_key = jax.random.fold_in(jax.random.key(seed), part)
    key_hidden, key_len, key_full = jax.random.split(part_key, 3)
    hidden = jax.random.normal(key_hidden, (N_SEQS, SEQ_LEN, D_MODEL), jnp.float32).astype(jnp.bfloat16)
    drawn_len = jax.random.randint(key_len, (N_SEQS,), max(1, SEQ_LEN // 8), SEQ_LEN + 1)
    full_idx = jax.random.randint(key_full, (), 0, N_SEQS)
    lengths = jnp.where(jnp.arange(N_SEQS) == full_idx, SEQ_LEN, drawn_len).astype(jnp.int32)
    weight_keys = jax.random.split(jax.random.key(seed + 1), 9)
    q_width = N_HEADS * HEAD_DIM
    kv_width = KV_HEADS * HEAD_DIM
    d_scale = D_MODEL ** -0.5
    return {
        'hidden': hidden,
        'lengths': lengths,
        'attn_norm': weight_draw(weight_keys[0], (N_LAYERS, D_MODEL), 0.5),
        'w_q': weight_draw(weight_keys[1], (N_LAYERS, D_MODEL, q_width), 1.5 * d_scale),
        'w_k': weight_draw(weight_keys[2], (N_LAYERS, D_MODEL, kv_width), 1.5 * d_scale),
        'w_v': weight_draw(weight_keys[3], (N_LAYERS, D_MODEL, kv_width), d_scale),
        'w_o': weight_draw(weight_keys[4], (N_LAYERS, q_width, D_MODEL), q_width ** -0.5),
        'mlp_norm': weight_draw(weight_keys[5], (N_LAYERS, D_MODEL), 0.5),
        'w_gate': weight_draw(weight_keys[6], (N_LAYERS, D_MODEL, D_FF), d_scale),
        'w_up': weight_draw(weight_keys[7], (N_LAYERS, D_MODEL, D_FF), d_scale),
        'w_down': weight_draw(weight_keys[8], (N_LAYERS, D_FF, D_MODEL), D_FF ** -0.5),
    }


def rms_norm(hidden_f, norm_gain):
    mean_sq = jnp.mean(hidden_f * hidden_f, axis=-1, keepdims=True)
    return (hidden_f * lax.rsqrt(mean_sq + RMS_EPS) * (1.0 + norm_gain.astype(jnp.float32))).astype(jnp.bfloat16)


def rope_tables():
    half_dim = HEAD_DIM // 2
    inv_freq = ROPE_THETA ** (-2.0 * jnp.arange(half_dim, dtype=jnp.float32) / HEAD_DIM)
    angles = jnp.arange(SEQ_LEN, dtype=jnp.float32)[:, None] * inv_freq[None, :]
    return jnp.cos(angles)[:, None, :], jnp.sin(angles)[:, None, :]


def apply_rope(projected, cos_tab, sin_tab):
    half_dim = HEAD_DIM // 2
    first_half = projected[..., :half_dim]
    second_half = projected[..., half_dim:]
    return jnp.concatenate([first_half * cos_tab - second_half * sin_tab, second_half * cos_tab + first_half * sin_tab], axis=-1)


def seq_attention(q_rope, k_rope, v_proj, length):
    key_pos = jnp.arange(SEQ_LEN)
    keys_f = k_rope.astype(jnp.float32)
    values_f = v_proj.astype(jnp.float32)

    def one_block(block_idx):
        q_start = block_idx * QUERY_BLOCK
        q_blk = lax.dynamic_slice_in_dim(q_rope, q_start, QUERY_BLOCK, 0).astype(jnp.float32)
        q_pos = q_start + jnp.arange(QUERY_BLOCK)
        scores = jnp.einsum('qhgd,shd->hgqs', q_blk, keys_f)
        allowed = (key_pos[None, :] <= q_pos[:, None]) & (key_pos[None, :] < length)
        scores = jnp.where(allowed, scores, -1e30)
        scores = scores - jnp.max(scores, axis=-1, keepdims=True)
        exp_scores = jnp.exp(scores)
        attn_probs = exp_scores / jnp.sum(exp_scores, axis=-1, keepdims=True)
        attn_probs = jnp.where((q_pos < length)[:, None], attn_probs, 0.0).astype(jnp.bfloat16)
        return jnp.einsum('hgqs,shd->qhgd', attn_probs.astype(jnp.float32), values_f).astype(jnp.bfloat16)

    blocks = lax.map(one_block, jnp.arange(SEQ_LEN // QUERY_BLOCK))
    return blocks.reshape(SEQ_LEN, N_HEADS * HEAD_DIM)


def one_layer(hidden, length, params):
    attn_gain, wq_layer, wk_layer, wv_layer, wo_layer, mlp_gain, wg_layer, wu_layer, wd_layer = params
    cos_tab, sin_tab = rope_tables()
    hidden_f = hidden.astype(jnp.float32)
    normed = rms_norm(hidden_f, attn_gain)
    q_proj = jnp.dot(normed, wq_layer, preferred_element_type=jnp.float32).reshape(SEQ_LEN, N_HEADS, HEAD_DIM)
    k_proj = jnp.dot(normed, wk_layer, preferred_element_type=jnp.float32).reshape(SEQ_LEN, KV_HEADS, HEAD_DIM)
    v_proj = jnp.dot(normed, wv_layer, preferred_element_type=jnp.float32).astype(jnp.bfloat16).reshape(SEQ_LEN, KV_HEADS, HEAD_DIM)
    q_rope = (apply_rope(q_proj, cos_tab, sin_tab) * HEAD_DIM ** -0.5).astype(jnp.bfloat16).reshape(SEQ_LEN, KV_HEADS, GROUP_SIZE, HEAD_DIM)
    k_rope = apply_rope(k_proj, cos_tab, sin_tab).astype(jnp.bfloat16)
    attn_out = seq_attention(q_rope, k_rope, v_proj, length)
    mixed_bf = (hidden_f + jnp.dot(attn_out, wo_layer, preferred_element_type=jnp.float32)).astype(jnp.bfloat16)
    mixed_f = mixed_bf.astype(jnp.float32)
    normed_mlp = rms_norm(mixed_f, mlp_gain)
    gate_proj = jnp.dot(normed_mlp, wg_layer, preferred_element_type=jnp.float32)
    up_proj = jnp.dot(normed_mlp, wu_layer, preferred_element_type=jnp.float32)
    act_bf = (jax.nn.gelu(gate_proj, approximate=True) * up_proj).astype(jnp.bfloat16)
    new_hidden = (mixed_f + jnp.dot(act_bf, wd_layer, preferred_element_type=jnp.float32)).astype(jnp.bfloat16)
    return new_hidden, k_rope, v_proj


def reference(hidden, lengths, attn_norm, w_q, w_k, w_v, w_o, mlp_norm, w_gate, w_up, w_down):
    stacked = (attn_norm, w_q, w_k, w_v, w_o, mlp_norm, w_gate, w_up, w_down)

    def one_seq(seq_args):
        seq_hidden, length = seq_args

        def layer_step(carry_hidden, params):
            new_hidden, k_rope, v_proj = one_layer(carry_hidden, length, params)
            return new_hidden, (k_rope, v_proj)

        final_hidden, kv_pair = lax.scan(layer_step, seq_hidden, stacked)
        return final_hidden, kv_pair[0], kv_pair[1]

    out_hidden, k_all, v_all = lax.map(one_seq, (hidden, lengths))
    return out_hidden, jnp.transpose(k_all, (1, 0, 2, 3, 4)), jnp.transpose(v_all, (1, 0, 2, 3, 4))
```

```python
import functools

import jax
import jax.numpy as jnp
from jax import lax
from jax.experimental import pallas as pl
from jax.experimental.pallas import tpu as pltpu
from jax.sharding import PartitionSpec as P

HEAD_DIM = 256
RMS_EPS = 1e-6
ROPE_THETA = 10000.0
N_DEV = 8
CHUNKS = 16
CORE, XAX, YAX = 1, 2, 4
TILE = 512
PRE = (1, 3)
EXTRA = (1, 0)
MESH = pl.DeviceIdType.MESH
TO_X, TO_Y, TO_C, FWD_X, FWD_Y, C_X, C_Y, C_D = range(8)
KINDS = 8


def rms_norm(hidden_f, norm_gain):
    mean_sq = jnp.mean(hidden_f * hidden_f, axis=-1, keepdims=True)
    return (hidden_f * lax.rsqrt(mean_sq + RMS_EPS) * (1.0 + norm_gain.astype(jnp.float32))).astype(jnp.bfloat16)


def rope_tables(seq_len):
    half_dim = HEAD_DIM // 2
    inv_freq = ROPE_THETA ** (-2.0 * jnp.arange(half_dim, dtype=jnp.float32) / HEAD_DIM)
    angles = jnp.arange(seq_len, dtype=jnp.float32)[:, None] * inv_freq[None, :]
    return jnp.cos(angles)[:, None, :], jnp.sin(angles)[:, None, :]


def apply_rope(projected, cos_tab, sin_tab):
    half_dim = HEAD_DIM // 2
    first_half = projected[..., :half_dim]
    second_half = projected[..., half_dim:]
    return jnp.concatenate([first_half * cos_tab - second_half * sin_tab, second_half * cos_tab + first_half * sin_tab], axis=-1)


def attention(q_rope, k_rope, v_proj, lengths):
    seq_len = q_rope.shape[1]
    scores = jnp.einsum('bqhgd,bshd->bhgqs', q_rope, k_rope, preferred_element_type=jnp.float32)
    pos = jnp.arange(seq_len)
    allowed = (pos[None, None, :] <= pos[None, :, None]) & (pos[None, None, :] < lengths[:, None, None])
    scores = jnp.where(allowed[:, None, None], scores, -1e30)
    scores = scores - jnp.max(scores, axis=-1, keepdims=True)
    exp_scores = jnp.exp(scores)
    attn_probs = exp_scores / jnp.sum(exp_scores, axis=-1, keepdims=True)
    row_live = pos[None, :] < lengths[:, None]
    attn_probs = jnp.where(row_live[:, None, None, :, None], attn_probs, 0.0).astype(jnp.bfloat16)
    return jnp.einsum('bhgqs,bshd->bqhgd', attn_probs, v_proj, preferred_element_type=jnp.float32).astype(jnp.bfloat16)


def attn_block(hidden, lengths, gain, w_qkv, w_o):
    n_seq, seq_len, d_model = hidden.shape
    q_width = w_o.shape[0]
    n_heads = q_width // HEAD_DIM
    cos_tab, sin_tab = rope_tables(seq_len)
    hidden_f = hidden.astype(jnp.float32)
    normed = rms_norm(hidden_f, gain)
    proj = jnp.einsum('bsd,de->bse', normed, w_qkv, preferred_element_type=jnp.float32)
    q_proj = proj[..., :q_width].reshape(n_seq, seq_len, n_heads, HEAD_DIM)
    k_proj = proj[..., q_width:q_width + HEAD_DIM].reshape(n_seq, seq_len, 1, HEAD_DIM)
    v_proj = proj[..., q_width + HEAD_DIM:].astype(jnp.bfloat16).reshape(n_seq, seq_len, 1, HEAD_DIM)
    q_rope = (apply_rope(q_proj, cos_tab, sin_tab) * HEAD_DIM ** -0.5).astype(jnp.bfloat16).reshape(n_seq, seq_len, 1, n_heads, HEAD_DIM)
    k_rope = apply_rope(k_proj, cos_tab, sin_tab).astype(jnp.bfloat16)
    attn_out = attention(q_rope, k_rope, v_proj, lengths).reshape(n_seq, seq_len, q_width)
    mixed = (hidden_f + jnp.einsum('bse,ed->bsd', attn_out, w_o, preferred_element_type=jnp.float32)).astype(jnp.bfloat16)
    return mixed, k_rope, v_proj


def mlp_kernel(layer, n_ext, n_pre, n_own, n_extra, ext_at, wg_ref, wu_ref, wd_ref, pre_ref, ext_ref, m_ref, gain_ref, out_ref, gat_ref,
               acc, r2, wbuf, stage, ssem, rsem, ldsem, iosem):
    me = lax.axis_index('w')
    depth = wg_ref.shape[1]
    width = r2.shape[1]
    n_tok = r2.shape[0]
    rows, cols = wbuf.shape[1:]
    half = rows // 2
    wide = cols // N_DEV
    n_ready = n_ext + n_pre
    n_comm = n_own + n_extra
    n_steps = n_ready + n_own

    barrier = pltpu.get_barrier_semaphore()
    for axis in (CORE, XAX, YAX):
        pl.semaphore_signal(barrier, inc=1, device_id={'w': me ^ axis}, device_id_type=MESH)
    pl.semaphore_wait(barrier, 3)

    def remote(src, dst, kind, k, axis):
        return pltpu.make_async_remote_copy(src_ref=src, dst_ref=dst, send_sem=ssem.at[kind, k], recv_sem=rsem.at[kind, k],
                                            device_id={'w': me ^ axis}, device_id_type=MESH)

    def rcopy(kind, k):
        if kind in (TO_X, TO_Y, TO_C):
            src, axis = gat_ref.at[k, me], {TO_X: XAX, TO_Y: YAX, TO_C: CORE}[kind]
        elif kind == FWD_X:
            src, axis = gat_ref.at[k, me ^ YAX, pl.ds(0, half)], XAX
        elif kind == FWD_Y:
            src, axis = gat_ref.at[k, me ^ XAX, pl.ds(half, half)], YAX
        else:
            src, axis = gat_ref.at[k, me ^ {C_X: XAX, C_Y: YAX, C_D: XAX | YAX}[kind]], CORE
        return remote(src, src, kind, k, axis)

    def own_parts(lay, chunk, dst, put):
        def column_block(j, carry):
            at = pl.ds(pl.multiple_of(j * (wide * CHUNKS) + chunk * wide, wide), wide)
            to = pl.ds(pl.multiple_of(j * wide, wide), wide)
            put(wg_ref.at[lay, :, at], dst.at[pl.ds(0, depth), to])
            put(wu_ref.at[lay, :, at], dst.at[pl.ds(depth, depth), to])
            return carry

        lax.fori_loop(0, N_DEV, column_block, 0)
        down = pl.ds(pl.multiple_of(chunk * wide, wide), wide)
        for side in range(2):
            put(wd_ref.at[lay, down, pl.ds(side * cols, cols)], dst.at[pl.ds(2 * depth + side * wide, wide)])

    def chunk_of(k):
        if isinstance(k, int):
            return (layer, n_ready + k) if k < n_own else (layer + 1, k - n_own)
        if n_extra == 0:
            return layer, n_ready + k
        return jnp.where(k < n_own, layer, layer + 1), jnp.where(k < n_own, n_ready + k, k - n_own)

    def stage_a(k):
        lay, chunk = chunk_of(k)
        for kind, axis in ((TO_X, XAX), (TO_Y, YAX), (TO_C, CORE)):
            own_parts(lay, chunk, gat_ref.at[k, me], lambda src, dst: remote(src, dst, kind, k, axis).start())

    def stage_b(k):
        rcopy(TO_X, k).wait_recv()
        rcopy(FWD_Y, k).start()
        rcopy(C_X, k).start()
        rcopy(TO_Y, k).wait_recv()
        rcopy(FWD_X, k).start()
        rcopy(C_Y, k).start()

    def stage_c(k):
        rcopy(FWD_X, k).wait_recv()
        rcopy(FWD_Y, k).wait_recv()
        rcopy(C_D, k).start()
        for kind in (TO_C, C_X, C_Y, C_D):
            rcopy(kind, k).wait_recv()

    def load_gathered(ref, at, chunk):
        own_parts(layer, chunk, wbuf.at[me], lambda src, dst: pltpu.make_async_copy(src, dst, ldsem).start())
        for delta in range(1, N_DEV):
            pltpu.make_async_copy(ref.at[at, me ^ delta], wbuf.at[me ^ delta], ldsem).start()

    def event_at(s):
        if n_ready == 1:
            return s
        event = s + 1 - n_ready
        early = {1: 0, 2: 1, 4: 2, 5: 3}
        for at in range(n_ready + 3):
            event = jnp.where(s == at, early.get(at, -1), event)
        return event

    stage_a(0)
    stage_a(1)

    gain = 1.0 + gain_ref[...]

    def norm_tile(i, carry):
        tok = pl.ds(pl.multiple_of(i * TILE, TILE), TILE)
        copy = pltpu.make_async_copy(m_ref.at[tok], stage, iosem)
        copy.start()
        copy.wait()
        m_f = stage[...].astype(jnp.float32)
        acc[tok, :] = m_f
        mean_sq = jnp.mean(m_f * m_f, axis=-1, keepdims=True)
        r2[tok, :] = (m_f * lax.rsqrt(mean_sq + RMS_EPS) * gain).astype(jnp.bfloat16)
        return carry

    lax.fori_loop(0, n_tok // TILE, norm_tile, 0)

    def step(s, carry):
        k = s - n_ready
        last = s == n_steps - 1

        event = event_at(s)

        @pl.when((event >= 0) & (event < n_comm))
        def _():
            stage_b(event)

        @pl.when((event >= 0) & (event + 2 < n_comm))
        def _():
            stage_a(event + 2)

        @pl.when(event >= 1)
        def _():
            stage_c(event - 1)

        @pl.when(k >= 0)
        def _():
            load_gathered(gat_ref, k, s)

        if n_ext:
            @pl.when(s < n_ext)
            def _():
                load_gathered(ext_ref, ext_at + s, s)

        if n_pre:
            @pl.when((s >= n_ext) & (s < n_ready))
            def _():
                for dev in range(N_DEV):
                    pltpu.make_async_copy(pre_ref.at[dev, s - n_ext], wbuf.at[dev], ldsem).start()

        pltpu.make_async_copy(gat_ref.at[0], wbuf, ldsem).wait()

        def tile_step(i, inner):
            tok = pl.ds(pl.multiple_of(i * TILE, TILE), TILE)
            r_t = r2[tok, :]
            gate = jnp.dot(r_t, wbuf[:, 0:depth, :].reshape(width, cols), preferred_element_type=jnp.float32)
            up = jnp.dot(r_t, wbuf[:, depth:2 * depth, :].reshape(width, cols), preferred_element_type=jnp.float32)
            act = (jax.nn.gelu(gate, approximate=True) * up).astype(jnp.bfloat16)
            for side in range(2):
                lo = 2 * depth + side * wide
                w_down = wbuf[:, lo:lo + wide, :].reshape(N_DEV * wide, cols)
                acc[tok, pl.ds(side * cols, cols)] += jnp.dot(act, w_down, preferred_element_type=jnp.float32)

            @pl.when(last)
            def _():
                @pl.when(i > 0)
                def _():
                    pltpu.make_async_copy(stage, out_ref.at[tok], iosem).wait()
                stage[...] = acc[tok, :].astype(jnp.bfloat16)
                pltpu.make_async_copy(stage, out_ref.at[tok], iosem).start()
            return inner

        lax.fori_loop(0, n_tok // TILE, tile_step, 0)
        return carry

    lax.fori_loop(0, n_steps, step, 0)
    pltpu.make_async_copy(stage, out_ref.at[pl.ds(0, TILE)], iosem).wait()

    for k in range(n_own, n_comm):
        if k > n_own:
            stage_b(k)
        stage_c(k)

    def drain(k, carry):
        for kind in range(KINDS):
            rcopy(kind, k).wait_send()
        return carry

    lax.fori_loop(0, n_comm, drain, 0)


def mlp_call(layer, w_gate, w_up, w_down, pre, ext, ext_at, mixed, gain):
    n_seq, seq_len, d_model = mixed.shape
    n_tok = n_seq * seq_len
    d_ff = w_gate.shape[2]
    depth = w_gate.shape[1]
    cols = d_ff // CHUNKS
    rows = 2 * depth + 2 * cols // N_DEV
    n_ext = EXTRA[layer - 1] if layer > 0 else 0
    n_extra = EXTRA[layer]
    n_pre = PRE[layer]
    n_own = CHUNKS - n_ext - n_pre
    out, gathered = pl.pallas_call(
        functools.partial(mlp_kernel, layer, n_ext, n_pre, n_own, n_extra, ext_at),
        out_shape=(jax.ShapeDtypeStruct((n_tok, d_model), jnp.bfloat16),
                   jax.ShapeDtypeStruct((n_own + n_extra, N_DEV, rows, cols), jnp.bfloat16)),
        in_specs=[pl.BlockSpec(memory_space=pl.ANY)] * 6 + [pl.BlockSpec(memory_space=pltpu.VMEM)],
        out_specs=[pl.BlockSpec(memory_space=pl.ANY)] * 2,
        scratch_shapes=[
            pltpu.VMEM((n_tok, d_model), jnp.float32),
            pltpu.VMEM((n_tok, d_model), jnp.bfloat16),
            pltpu.VMEM((N_DEV, rows, cols), jnp.bfloat16),
            pltpu.VMEM((TILE, d_model), jnp.bfloat16),
            pltpu.SemaphoreType.DMA((KINDS, n_own + n_extra)),
            pltpu.SemaphoreType.DMA((KINDS, n_own + n_extra)),
            pltpu.SemaphoreType.DMA,
            pltpu.SemaphoreType.DMA,
        ],
        compiler_params=pltpu.CompilerParams(collective_id=layer, has_side_effects=True, vmem_limit_bytes=63 * 1024 * 1024),
        cost_estimate=pl.CostEstimate(flops=6 * n_tok * d_model * d_ff, bytes_accessed=12 * d_model * d_ff, transcendentals=0),
        name=f'mlp_gather_{layer}',
    )(w_gate, w_up, w_down, pre, ext, mixed.reshape(n_tok, d_model), (gain.astype(jnp.float32)).reshape(1, d_model))
    return out.reshape(n_seq, seq_len, d_model), gathered, n_own


def pack_kernel(layer, first, wg_ref, wu_ref, wd_ref, out_ref, sem):
    depth = wg_ref.shape[1]
    count, _, cols = out_ref.shape
    wide = cols // N_DEV
    for i in range(count):
        chunk = first + i
        for j in range(N_DEV):
            at = pl.ds(j * wide * CHUNKS + chunk * wide, wide)
            to = pl.ds(j * wide, wide)
            pltpu.make_async_copy(wg_ref.at[layer, :, at], out_ref.at[i, pl.ds(0, depth), to], sem).start()
            pltpu.make_async_copy(wu_ref.at[layer, :, at], out_ref.at[i, pl.ds(depth, depth), to], sem).start()
        for side in range(2):
            src = wd_ref.at[layer, pl.ds(chunk * wide, wide), pl.ds(side * cols, cols)]
            pltpu.make_async_copy(src, out_ref.at[i, pl.ds(2 * depth + side * wide, wide)], sem).start()
    pltpu.make_async_copy(out_ref, out_ref, sem).wait()


def own_pieces(layer, first, count, w_gate, w_up, w_down):
    depth = w_gate.shape[1]
    cols = w_gate.shape[2] // CHUNKS
    rows = 2 * depth + 2 * cols // N_DEV
    return pl.pallas_call(
        functools.partial(pack_kernel, layer, first),
        out_shape=jax.ShapeDtypeStruct((count, rows, cols), jnp.bfloat16),
        in_specs=[pl.BlockSpec(memory_space=pl.ANY)] * 3,
        out_specs=pl.BlockSpec(memory_space=pltpu.VMEM),
        scratch_shapes=[pltpu.SemaphoreType.DMA],
        name=f'pack_{layer}',
    )(w_gate, w_up, w_down)


def solution(mesh):
    batch_spec = P(('dp', 'w'))
    weight_spec = P(None, 'w')
    cache_spec = P(None, ('dp', 'w'))

    def device_fn(hidden, lengths, attn_norm, w_q, w_k, w_v, w_o, mlp_norm, w_gate, w_up, w_down):
        n_layers = w_q.shape[0]
        gains = lax.all_gather(jnp.concatenate([attn_norm, mlp_norm], axis=0), 'w', axis=1, tiled=True)
        k_list = []
        v_list = []
        ext, ext_at = None, 0
        for layer in range(n_layers):
            qkv_own = jnp.concatenate([w_q[layer], w_k[layer], w_v[layer]], axis=1)
            w_qkv_full = lax.all_gather(qkv_own, 'w', axis=0, tiled=True)
            w_o_full = lax.all_gather(w_o[layer], 'w', axis=0, tiled=True)
            n_ext = EXTRA[layer - 1] if layer > 0 else 0
            pre_own = own_pieces(layer, n_ext, PRE[layer], w_gate, w_up, w_down)
            if layer > 0:
                pre_own, hidden = lax.optimization_barrier((pre_own, hidden))
            pre = lax.all_gather(pre_own, 'w', axis=0, tiled=False)
            mixed, k_rope, v_proj = attn_block(hidden, lengths, gains[layer], w_qkv_full, w_o_full)
            hidden, ext, ext_at = mlp_call(layer, w_gate, w_up, w_down, pre, pre if ext is None else ext, ext_at, mixed, gains[n_layers + layer])
            k_list.append(k_rope)
            v_list.append(v_proj)
        return hidden, jnp.stack(k_list), jnp.stack(v_list)

    return jax.shard_map(device_fn, mesh=mesh, in_specs=(batch_spec, batch_spec) + (weight_spec,) * 9, out_specs=(batch_spec, cache_spec, cache_spec), check_vma=False)
```

```python
import functools

import jax
import jax.numpy as jnp
from jax import lax
from jax.experimental import pallas as pl
from jax.experimental.pallas import tpu as pltpu
from jax.sharding import PartitionSpec as P

HEAD_DIM = 256
RMS_EPS = 1e-6
ROPE_THETA = 10000.0
N_DEV = 8
CHUNKS = 16
CORE, XAX, YAX = 1, 2, 4
TILE = 512
PRE = 2
GAIN_ROWS = 8
MESH = pl.DeviceIdType.MESH
TO_X, TO_Y, TO_C, FWD_X, FWD_Y, C_X, C_Y, C_D = range(8)
KINDS = 8


def rope_tables(seq_len):
    half_dim = HEAD_DIM // 2
    inv_freq = ROPE_THETA ** (-2.0 * jnp.arange(half_dim, dtype=jnp.float32) / HEAD_DIM)
    angles = jnp.arange(seq_len, dtype=jnp.float32)[:, None] * inv_freq[None, :]
    return jnp.cos(angles), jnp.sin(angles)


class Gather:
    def __init__(self, gat_ref, ssem, rsem, half):
        self.me = lax.axis_index('w')
        self.gat, self.ssem, self.rsem, self.half = gat_ref, ssem, rsem, half

    def remote(self, src, dst, kind, k, axis):
        return pltpu.make_async_remote_copy(src_ref=src, dst_ref=dst, send_sem=self.ssem.at[kind, k], recv_sem=self.rsem.at[kind, k],
                                            device_id={'w': self.me ^ axis}, device_id_type=MESH)

    def rcopy(self, kind, k):
        me, half = self.me, self.half
        if kind in (TO_X, TO_Y, TO_C):
            src, axis = self.gat.at[k, me], {TO_X: XAX, TO_Y: YAX, TO_C: CORE}[kind]
        elif kind == FWD_X:
            src, axis = self.gat.at[k, me ^ YAX, pl.ds(0, half)], XAX
        elif kind == FWD_Y:
            src, axis = self.gat.at[k, me ^ XAX, pl.ds(half, self.gat.shape[2] - half)], YAX
        else:
            src, axis = self.gat.at[k, me ^ {C_X: XAX, C_Y: YAX, C_D: XAX | YAX}[kind]], CORE
        return self.remote(src, src, kind, k, axis)

    def stage_a(self, k, parts):
        for kind, axis in ((TO_X, XAX), (TO_Y, YAX), (TO_C, CORE)):
            parts(self.gat.at[k, self.me], lambda src, dst: self.remote(src, dst, kind, k, axis).start())

    def stage_b(self, k):
        self.rcopy(TO_X, k).wait_recv()
        self.rcopy(FWD_Y, k).start()
        self.rcopy(C_X, k).start()
        self.rcopy(TO_Y, k).wait_recv()
        self.rcopy(FWD_X, k).start()
        self.rcopy(C_Y, k).start()

    def stage_c(self, k):
        self.rcopy(FWD_X, k).wait_recv()
        self.rcopy(FWD_Y, k).wait_recv()
        self.rcopy(C_D, k).start()
        for kind in (TO_C, C_X, C_Y, C_D):
            self.rcopy(kind, k).wait_recv()

    def drain(self, count):
        def one(k, carry):
            for kind in range(KINDS):
                self.rcopy(kind, k).wait_send()
            return carry

        lax.fori_loop(0, count, one, 0)


def greet():
    barrier = pltpu.get_barrier_semaphore()
    for axis in (CORE, XAX, YAX):
        pl.semaphore_signal(barrier, inc=1, device_id={'w': lax.axis_index('w') ^ axis}, device_id_type=MESH)
    pl.semaphore_wait(barrier, 3)


def chunk_parts(layer, chunk, mlp_refs, dst, put):
    wg_ref, wu_ref, wd_ref = mlp_refs
    depth, cols = wg_ref.shape[1], wg_ref.shape[2] // CHUNKS
    wide = cols // N_DEV

    def column_block(j, carry):
        at = pl.ds(pl.multiple_of(j * (wide * CHUNKS) + chunk * wide, wide), wide)
        to = pl.ds(pl.multiple_of(j * wide, wide), wide)
        put(wg_ref.at[layer, :, at], dst.at[pl.ds(0, depth), to])
        put(wu_ref.at[layer, :, at], dst.at[pl.ds(depth, depth), to])
        return carry

    lax.fori_loop(0, N_DEV, column_block, 0)
    down = pl.ds(pl.multiple_of(chunk * wide, wide), wide)
    for side in range(2):
        put(wd_ref.at[layer, down, pl.ds(side * cols, cols)], dst.at[pl.ds(2 * depth + side * wide, wide)])


def attn_parts(layer, attn_refs, dst, put):
    at = 0
    depth = attn_refs[0].shape[1]
    for ref in attn_refs[:-1]:
        put(ref.at[layer], dst.at[pl.ds(0, depth), pl.ds(at, ref.shape[2])])
        at += ref.shape[2]
    put(attn_refs[-1], dst.at[pl.ds(depth, GAIN_ROWS)])


def attn_kernel(layer, n_layers, len_ref, wg_ref, wu_ref, wd_ref, wq_ref, wk_ref, wv_ref, wo_ref, ng_ref, full_ref, h_ref, cos_ref, sin_ref,
                m_ref, k_ref, v_ref, gain_ref, gat_ref, *rest):
    if layer == 0:
        attn_gat, w_v, h_v, m_v, o_v, ssem, rsem, wsem, hsem, msem, att_s, att_r = rest
    else:
        w_v, h_v, m_v, o_v, ssem, rsem, wsem, hsem, msem = rest
        attn_gat = full_ref
    me = lax.axis_index('w')
    count = gat_ref.shape[0]
    n_seq, seq_len, head_dim = k_ref.shape
    q_width = o_v.shape[1]
    d_model = h_v.shape[1]
    depth = wq_ref.shape[1]
    half = head_dim // 2
    mlp_refs = wg_ref, wu_ref, wd_ref
    attn_refs = wq_ref, wk_ref, wv_ref, wo_ref, ng_ref
    comm = Gather(gat_ref, ssem, rsem, gat_ref.shape[2] // 2)
    greet()
    load_h = pltpu.make_async_copy(h_ref, h_v, hsem)
    load_h.start()
    if layer == 0:
        first = Gather(attn_gat, att_s, att_r, depth // 2)
        first.stage_a(0, functools.partial(attn_parts, layer, attn_refs))
        first.stage_b(0)
    for k in range(count):
        comm.stage_a(k, functools.partial(chunk_parts, layer, k, mlp_refs))
    if layer == 0:
        first.stage_c(0)
    attn_parts(layer, attn_refs, w_v.at[me], lambda src, dst: pltpu.make_async_copy(src, dst, wsem).start())
    for delta in range(1, N_DEV):
        pltpu.make_async_copy(attn_gat.at[0, me ^ delta], w_v.at[me ^ delta], wsem).start()
    load_h.wait()
    pltpu.make_async_copy(attn_gat.at[0], w_v, wsem).wait()

    def gain_of(at):
        rows = [w_v[dev, depth:depth + GAIN_ROWS, 0:depth].astype(jnp.float32)[at:at + 1] for dev in range(N_DEV)]
        return jnp.concatenate(rows, axis=1)

    gain = 1.0 + gain_of(layer)
    gain_ref[...] = gain_of(n_layers + layer)
    row = lax.broadcasted_iota(jnp.int32, (seq_len, seq_len), 0)
    col = lax.broadcasted_iota(jnp.int32, (seq_len, seq_len), 1)

    def prompt(p, carry):
        @pl.when(p == 3)
        def _():
            comm.stage_b(0)

        @pl.when(p == 6)
        def _():
            comm.stage_b(1)
            comm.stage_c(0)

        tok = pl.ds(pl.multiple_of(p * seq_len, seq_len), seq_len)
        h_f = h_v[tok, :].astype(jnp.float32)
        mean_sq = jnp.mean(h_f * h_f, axis=-1, keepdims=True)
        normed = (h_f * lax.rsqrt(mean_sq + RMS_EPS) * gain).astype(jnp.bfloat16)
        cos, sin = cos_ref[...], sin_ref[...]

        def rope(x):
            a, c = x[:, :half], x[:, half:]
            return jnp.concatenate([a * cos - c * sin, c * cos + a * sin], axis=-1)

        kv = jnp.dot(normed, w_v[:, 0:depth, q_width:q_width + 2 * head_dim].reshape(d_model, 2 * head_dim), preferred_element_type=jnp.float32)
        k_rope = rope(kv[:, :head_dim]).astype(jnp.bfloat16)
        v_proj = kv[:, head_dim:].astype(jnp.bfloat16)
        k_ref[p] = k_rope
        v_ref[p] = v_proj
        length = len_ref[p]
        allowed = (col <= row) & (col < length)
        live = row < length
        for head in range(q_width // head_dim):
            at = slice(head * head_dim, (head + 1) * head_dim)
            q = jnp.dot(normed, w_v[:, 0:depth, at].reshape(d_model, head_dim), preferred_element_type=jnp.float32)
            q_rope = (rope(q) * head_dim ** -0.5).astype(jnp.bfloat16)
            scores = lax.dot_general(q_rope, k_rope, (((1,), (1,)), ((), ())), preferred_element_type=jnp.float32)
            scores = jnp.where(allowed, scores, -1e30)
            exp_scores = jnp.exp(scores - jnp.max(scores, axis=-1, keepdims=True))
            probs = exp_scores * (1.0 / jnp.sum(exp_scores, axis=-1, keepdims=True))
            probs = jnp.where(live, probs, 0.0).astype(jnp.bfloat16)
            o_v[:, at] = jnp.dot(probs, v_proj, preferred_element_type=jnp.float32).astype(jnp.bfloat16)
        w_o = w_v[:, 0:depth, q_width + 2 * head_dim:].reshape(q_width, d_model)
        mixed = h_f + jnp.dot(o_v[...], w_o, preferred_element_type=jnp.float32)
        m_v[tok, :] = mixed.astype(jnp.bfloat16)
        pltpu.make_async_copy(m_v.at[tok], m_ref.at[tok], msem.at[p]).start()
        return carry

    lax.fori_loop(0, n_seq, prompt, 0)
    comm.stage_c(1)
    for p in range(n_seq):
        tok = pl.ds(p * seq_len, seq_len)
        pltpu.make_async_copy(m_v.at[tok], m_ref.at[tok], msem.at[p]).wait()
    comm.drain(count)
    if layer == 0:
        first.drain(1)


def attn_call(layer, lengths, mlp_weights, attn_weights, full, hidden, seq_len):
    n_tok, d_model = hidden.shape
    n_seq = n_tok // seq_len
    w_gate, w_q = mlp_weights[0], attn_weights[0]
    n_layers, depth, q_width = w_q.shape
    cols = w_gate.shape[2] // CHUNKS
    rows = 2 * depth + 2 * cols // N_DEV
    piece = (depth + GAIN_ROWS, q_width + 2 * HEAD_DIM + d_model)
    cos_tab, sin_tab = rope_tables(seq_len)
    any_spec, vmem_spec = pl.BlockSpec(memory_space=pl.ANY), pl.BlockSpec(memory_space=pltpu.VMEM)
    out_shape = [jax.ShapeDtypeStruct((n_tok, d_model), jnp.bfloat16),
                 jax.ShapeDtypeStruct((n_seq, seq_len, HEAD_DIM), jnp.bfloat16),
                 jax.ShapeDtypeStruct((n_seq, seq_len, HEAD_DIM), jnp.bfloat16),
                 jax.ShapeDtypeStruct((1, d_model), jnp.float32),
                 jax.ShapeDtypeStruct((PRE, N_DEV, rows, cols), jnp.bfloat16)]
    out_specs = [any_spec, vmem_spec, vmem_spec, vmem_spec, any_spec]
    scratch = [
        pltpu.VMEM((N_DEV,) + piece, jnp.bfloat16),
        pltpu.VMEM((n_tok, d_model), jnp.bfloat16),
        pltpu.VMEM((n_tok, d_model), jnp.bfloat16),
        pltpu.VMEM((seq_len, q_width), jnp.bfloat16),
        pltpu.SemaphoreType.DMA((KINDS, PRE)),
        pltpu.SemaphoreType.DMA((KINDS, PRE)),
        pltpu.SemaphoreType.DMA,
        pltpu.SemaphoreType.DMA,
        pltpu.SemaphoreType.DMA((n_seq,)),
    ]
    if layer == 0:
        out_shape.append(jax.ShapeDtypeStruct((1, N_DEV) + piece, jnp.bfloat16))
        out_specs.append(any_spec)
        scratch += [pltpu.SemaphoreType.DMA((KINDS, 1))] * 2
        full = hidden
    return pl.pallas_call(
        functools.partial(attn_kernel, layer, n_layers),
        out_shape=out_shape,
        in_specs=[pl.BlockSpec(memory_space=pltpu.SMEM)] + [any_spec] * 10 + [vmem_spec] * 2,
        out_specs=out_specs,
        scratch_shapes=scratch,
        compiler_params=pltpu.CompilerParams(collective_id=2 + layer, has_side_effects=True, vmem_limit_bytes=63 * 1024 * 1024),
        cost_estimate=pl.CostEstimate(flops=2 * n_tok * d_model * piece[1], bytes_accessed=8 * n_tok * d_model, transcendentals=0),
        name=f'attn_gather_{layer}',
    )(lengths, *mlp_weights, *attn_weights, full, hidden, cos_tab, sin_tab)[:5]


def mlp_kernel(layer, n_own, n_layers, wg_ref, wu_ref, wd_ref, wq_ref, wk_ref, wv_ref, wo_ref, ng_ref, pre_ref, m_ref, gain_ref, out_ref, gat_ref, *rest):
    more = layer + 1 < n_layers
    if more:
        attn_gat, acc, r2, wbuf, stage, ssem, rsem, ldsem, iosem, att_s, att_r = rest
    else:
        acc, r2, wbuf, stage, ssem, rsem, ldsem, iosem = rest
    me = lax.axis_index('w')
    depth = wg_ref.shape[1]
    width = r2.shape[1]
    n_tok = r2.shape[0]
    cols = wbuf.shape[2]
    wide = cols // N_DEV
    n_steps = PRE + n_own
    mlp_refs = wg_ref, wu_ref, wd_ref
    attn_refs = wq_ref, wk_ref, wv_ref, wo_ref, ng_ref
    comm = Gather(gat_ref, ssem, rsem, gat_ref.shape[2] // 2)
    greet()
    if more:
        after = Gather(attn_gat, att_s, att_r, depth // 2)

    def stage_a(k):
        comm.stage_a(k, functools.partial(chunk_parts, layer, PRE + k, mlp_refs))

    def load_gathered(ref, at, chunk):
        chunk_parts(layer, chunk, mlp_refs, wbuf.at[me], lambda src, dst: pltpu.make_async_copy(src, dst, ldsem).start())
        for delta in range(1, N_DEV):
            pltpu.make_async_copy(ref.at[at, me ^ delta], wbuf.at[me ^ delta], ldsem).start()

    stage_a(0)
    stage_a(1)

    gain = 1.0 + gain_ref[...]

    def norm_tile(i, carry):
        tok = pl.ds(pl.multiple_of(i * TILE, TILE), TILE)
        copy = pltpu.make_async_copy(m_ref.at[tok], stage, iosem)
        copy.start()
        copy.wait()
        m_f = stage[...].astype(jnp.float32)
        acc[tok, :] = m_f
        mean_sq = jnp.mean(m_f * m_f, axis=-1, keepdims=True)
        r2[tok, :] = (m_f * lax.rsqrt(mean_sq + RMS_EPS) * gain).astype(jnp.bfloat16)
        return carry

    lax.fori_loop(0, n_tok // TILE, norm_tile, 0)

    def step(s, carry):
        k = s - PRE
        event = k + 1
        last = s == n_steps - 1
        tail = n_own - 1
        handled = n_own if more else tail

        @pl.when((event >= 0) & (event < handled))
        def _():
            comm.stage_b(event)

        if more:
            @pl.when((event >= 0) & (event + 2 < n_own))
            def _():
                stage_a(event + 2)

            @pl.when(event + 2 == n_own)
            def _():
                after.stage_a(0, functools.partial(attn_parts, layer + 1, attn_refs))

            @pl.when(event == n_own)
            def _():
                after.stage_b(0)
        else:
            @pl.when((event >= 0) & ((event + 2 < tail) | (event + 1 == tail)))
            def _():
                stage_a(jnp.where(event + 1 == tail, tail, event + 2))

        @pl.when(event >= 1)
        def _():
            comm.stage_c(event - 1)

        @pl.when(k >= 0)
        def _():
            load_gathered(gat_ref, k, s)

        @pl.when(k < 0)
        def _():
            load_gathered(pre_ref, s, s)

        pltpu.make_async_copy(gat_ref.at[0], wbuf, ldsem).wait()

        def tile_step(i, inner):
            tok = pl.ds(pl.multiple_of(i * TILE, TILE), TILE)
            if not more:
                @pl.when((event == tail) & (i == n_tok // TILE // 2))
                def _():
                    comm.stage_b(tail)

            r_t = r2[tok, :]
            gate = jnp.dot(r_t, wbuf[:, 0:depth, :].reshape(width, cols), preferred_element_type=jnp.float32)
            up = jnp.dot(r_t, wbuf[:, depth:2 * depth, :].reshape(width, cols), preferred_element_type=jnp.float32)
            act = (jax.nn.gelu(gate, approximate=True) * up).astype(jnp.bfloat16)
            for side in range(2):
                lo = 2 * depth + side * wide
                w_down = wbuf[:, lo:lo + wide, :].reshape(N_DEV * wide, cols)
                acc[tok, pl.ds(side * cols, cols)] += jnp.dot(act, w_down, preferred_element_type=jnp.float32)

            @pl.when(last)
            def _():
                @pl.when(i > 0)
                def _():
                    pltpu.make_async_copy(stage, out_ref.at[tok], iosem).wait()
                stage[...] = acc[tok, :].astype(jnp.bfloat16)
                pltpu.make_async_copy(stage, out_ref.at[tok], iosem).start()
            return inner

        lax.fori_loop(0, n_tok // TILE, tile_step, 0)
        return carry

    lax.fori_loop(0, n_steps, step, 0)
    pltpu.make_async_copy(stage, out_ref.at[pl.ds(0, TILE)], iosem).wait()

    if more:
        after.stage_c(0)
        after.drain(1)
    comm.drain(n_own)


def mlp_call(layer, mlp_weights, attn_weights, pre, mixed, gain):
    n_tok, d_model = mixed.shape
    n_layers, depth, d_ff = mlp_weights[0].shape
    cols = d_ff // CHUNKS
    rows = 2 * depth + 2 * cols // N_DEV
    n_own = CHUNKS - PRE
    any_spec = pl.BlockSpec(memory_space=pl.ANY)
    out_shape = [jax.ShapeDtypeStruct((n_tok, d_model), jnp.bfloat16),
                 jax.ShapeDtypeStruct((n_own, N_DEV, rows, cols), jnp.bfloat16)]
    scratch = [
        pltpu.VMEM((n_tok, d_model), jnp.float32),
        pltpu.VMEM((n_tok, d_model), jnp.bfloat16),
        pltpu.VMEM((N_DEV, rows, cols), jnp.bfloat16),
        pltpu.VMEM((TILE, d_model), jnp.bfloat16),
        pltpu.SemaphoreType.DMA((KINDS, n_own)),
        pltpu.SemaphoreType.DMA((KINDS, n_own)),
        pltpu.SemaphoreType.DMA,
        pltpu.SemaphoreType.DMA,
    ]
    if layer + 1 < n_layers:
        width = sum(weight.shape[2] for weight in attn_weights[:-1])
        out_shape.append(jax.ShapeDtypeStruct((1, N_DEV, depth + GAIN_ROWS, width), jnp.bfloat16))
        scratch += [pltpu.SemaphoreType.DMA((KINDS, 1))] * 2
    outs = pl.pallas_call(
        functools.partial(mlp_kernel, layer, n_own, n_layers),
        out_shape=out_shape,
        in_specs=[any_spec] * 10 + [pl.BlockSpec(memory_space=pltpu.VMEM)],
        out_specs=[any_spec] * len(out_shape),
        scratch_shapes=scratch,
        compiler_params=pltpu.CompilerParams(collective_id=layer, has_side_effects=True, vmem_limit_bytes=63 * 1024 * 1024),
        cost_estimate=pl.CostEstimate(flops=6 * n_tok * d_model * d_ff, bytes_accessed=12 * d_model * d_ff, transcendentals=0),
        name=f'mlp_gather_{layer}',
    )(*mlp_weights, *attn_weights, pre, mixed, gain)
    return outs[0], outs[-1]


def solution(mesh):
    batch_spec = P(('dp', 'w'))
    weight_spec = P(None, 'w')
    cache_spec = P(None, ('dp', 'w'))

    def device_fn(hidden, lengths, attn_norm, w_q, w_k, w_v, w_o, mlp_norm, w_gate, w_up, w_down):
        n_layers = w_q.shape[0]
        n_seq, seq_len, d_model = hidden.shape
        mlp_weights = (w_gate, w_up, w_down)
        width = sum(weight.shape[2] for weight in (w_q, w_k, w_v, w_o))
        own_gains = jnp.concatenate([attn_norm, mlp_norm], axis=0)
        own_gains = jnp.pad(own_gains, ((0, GAIN_ROWS - 2 * n_layers), (0, width - own_gains.shape[1])))
        attn_weights = (w_q, w_k, w_v, w_o, own_gains)
        k_list = []
        v_list = []
        full = None
        state = hidden.reshape(n_seq * seq_len, d_model)
        for layer in range(n_layers):
            mixed, k_rope, v_proj, gain, pre = attn_call(layer, lengths, mlp_weights, attn_weights, full, state, seq_len)
            state, full = mlp_call(layer, mlp_weights, attn_weights, pre, mixed, gain)
            k_list.append(k_rope[:, :, None, :])
            v_list.append(v_proj[:, :, None, :])
        return state.reshape(hidden.shape), jnp.stack(k_list), jnp.stack(v_list)

    return jax.shard_map(device_fn, mesh=mesh, in_specs=(batch_spec, batch_spec) + (weight_spec,) * 9, out_specs=(batch_spec, cache_spec, cache_spec), check_vma=False)
```
